32 devices in a mesh: cfg: 2 (over x), seq: 16 (over z, y, core).
Axes of the slice: x: 2, y: 2, z: 4, core: 2. Of those that a mesh axis runs over, the one named last changes fastest.
Arguments:
- latent: bfloat16 [16, 1024, 1536], P('seq'), may hold values from -6 to 6
- text_ids: int32 [2, 512], P('cfg'), may hold values from 0 to 32127
- timestep: int32 [1], replicated, may hold values from 0 to 999
- guide_num: int32 [1], replicated, may hold values from 1024 to 8192
- guide_den: int32 [1], replicated, may hold values from 512 to 1024
- text_table: bfloat16 [32128, 1536], P('seq'), may hold values from -6 to 6
- time_in: bfloat16 [256, 1536], replicated, may hold values from -0.375 to 0.375
- time_out: bfloat16 [1536, 1536], P(None, 'seq'), may hold values from -0.15625 to 0.15625
- mod_weight: bfloat16 [1536, 7680], P(None, 'seq'), may hold values from -0.109375 to 0.109375
- qkv_weight: bfloat16 [1536, 4608], replicated, may hold values from -1 to 1
- out_weight: bfloat16 [1536, 1536], replicated, may hold values from -0.625 to 0.625
- head_weight: bfloat16 [1536, 64], replicated, may hold values from -0.15625 to 0.15625
Outputs:
- guided: float32 [16, 1024, 64], P('seq')
The draws below stay inside these ranges and needn't reach their ends.
All inputs are finite; a program needn't handle non-finite values.
Results may differ from the reference program's by a relative error of at most 0.0117.
Values may be sent and summed in bfloat16 or wider, within the bound.
No kernel may reach another device: no remote copies, remote signals or barrier semaphores. Data moves between devices by JAX's collectives and lax.ppermute only.
A program may use at most 128 MiB of HBM per device.

```python
import math
import jax
import jax.numpy as jnp
import numpy as np
from jax import lax

D = 1536
HEADS = 24
OUT_CH = 64
VOCAB = 32128
FREQ = 256
TEXT = 512
PIXELS = 1024
FRAMES = 16
N_SEQ = 16


def draw_qkv_weight(key, part):
    base_key, head_key = jax.random.split(jax.random.fold_in(key, 17))
    spread_scale = 1.0 / math.sqrt(D)
    entries = jax.random.truncated_normal(base_key, -4.0, 4.0, (D, 3 * D), jnp.float32) * spread_scale
    return jnp.clip(entries, -1.0, 1.0).astype(jnp.bfloat16)


def touch_ends(result, stream_key, least, top_value):
    longest = result.shape.index(max(result.shape))
    spots = []
    for shift in (0, 1):
        where = [jax.random.randint(jax.random.fold_in(stream_key, axis), (), 0, length) for axis, length in enumerate(result.shape)]
        where[longest] = (where[longest] + shift) % result.shape[longest]
        spots.append(tuple(where))
    return result.at[spots[0]].set(least).at[spots[1]].set(top_value)


def block_levels(stream_key, dims, cuts, low, high):
    def one(dim, parts):
        heights = jax.random.uniform(jax.random.fold_in(jax.random.fold_in(stream_key, 6), dim), (parts,), jnp.float32, low / len(cuts), high / len(cuts))
        return jnp.repeat(jnp.exp(heights), dims[dim] // parts).reshape((-1,) + (1,) * (len(dims) - dim - 1))

    loudness = one(*cuts[0])
    for cut in cuts[1:]:
        loudness = loudness * one(*cut)
    return loudness


def rank_table(amount, skew):
    weights = [(1 << 20) // math.isqrt(rank ** skew) + 1 for rank in range(1, amount + 1)]
    width = 1 + sum(weights) // (1 << 30)
    return np.cumsum(np.array([max(1, weight // width) for weight in weights]))


def ranked(stream_key, dims, count, skew):
    table = rank_table(count, skew)
    pick = jax.random.randint(jax.random.fold_in(stream_key, 1), dims, 0, int(table[count - 1]))
    rank = jnp.searchsorted(jnp.asarray(table, jnp.int32), pick, side="right")
    return jax.random.permutation(jax.random.fold_in(stream_key, 2), count)[rank].astype(jnp.int32)


def scatter_about(rng, shape, scale, reach, shards=(), kind=jnp.bfloat16):
    drawn = jax.random.normal(rng, shape, jnp.float32) * scale
    if len(shards) > 0:
        drawn = block_levels(rng, shape, shards, -0.22, 0.18) * drawn
    return jnp.clip(drawn, min=-reach, max=reach).astype(kind)


def setup_inputs(seed: int = 0) -> dict:
    seeds = jax.random.split(jax.random.key(seed), 13)
    return {
        "latent": scatter_about(seeds[0], (FRAMES, PIXELS, D), 1.0, 6.0, ((0, 16),)),
        "text_ids": touch_ends(ranked(seeds[1], (2, TEXT), VOCAB, 1), jax.random.fold_in(seeds[1], 3), 0, VOCAB - 1).astype(jnp.int32),
        "timestep": jax.random.randint(seeds[2], (1,), 0, 1000).astype(jnp.int32),
        "guide_num": jax.random.randint(seeds[3], (1,), 1024, 8193).astype(jnp.int32),
        "guide_den": jax.random.randint(seeds[4], (1,), 512, 1025).astype(jnp.int32),
        "text_table": scatter_about(seeds[5], (VOCAB, D), 1.0, 6.0, ((0, 16),)),
        "time_in": scatter_about(seeds[6], (FREQ, D), FREQ ** -0.5, 0.375),
        "time_out": scatter_about(seeds[7], (D, D), D ** -0.5, 0.15625, ((1, 16),)),
        "mod_weight": scatter_about(seeds[8], (D, 5 * D), (2 * D) ** -0.5, 0.109375, ((1, 16),)),
        "qkv_weight": draw_qkv_weight(jax.random.fold_in(seeds[12], 71), 0),
        "out_weight": scatter_about(seeds[10], (D, D), (D // 16) ** -0.5, 0.625),
        "head_weight": scatter_about(seeds[11], (D, OUT_CH), D ** -0.5, 0.15625),
    }


norm_floor = 0.1

def layer_norm(values):
    center = values - lax.optimization_barrier(jnp.mean(values, axis=-1, keepdims=True))
    spread = lax.optimization_barrier(jnp.mean(center * center, axis=-1, keepdims=True))
    return center * lax.rsqrt(spread + norm_floor)

def modulate(values, shift_part, scale_part):
    return (layer_norm(values) * (1.0 + scale_part) + shift_part).astype(jnp.bfloat16)

def time_features(timestep):
    half_width = FREQ // 2
    ladder = jnp.arange(half_width, dtype=jnp.float32)
    freq_rates = jnp.exp(-math.log(10000.0) * ladder / half_width)
    angles = timestep.astype(jnp.float32)[0] * freq_rates
    return jnp.concatenate([jnp.cos(angles), jnp.sin(angles)])[None, :].astype(jnp.bfloat16)

def temporal_mix(normed, qkv_weight):
    frame_count, item_count, model_width = normed.shape
    head_dim = model_width // HEADS
    projected = jnp.dot(normed.reshape(-1, model_width), qkv_weight, preferred_element_type=jnp.float32)
    qkv_parts = []
    for part_index in range(3):
        rounded = projected[:, part_index * model_width:(part_index + 1) * model_width].astype(jnp.bfloat16)
        rounded = lax.optimization_barrier(rounded)
        qkv_parts.append(rounded.astype(jnp.float32).reshape(frame_count, item_count, HEADS, head_dim))
    scores = jnp.einsum('fphd,gphd->phfg', qkv_parts[0], qkv_parts[1]) * (1.0 / math.sqrt(head_dim))
    attn_prob = lax.optimization_barrier(jax.nn.softmax(scores, axis=-1).astype(jnp.bfloat16))
    mixed_rows = jnp.einsum('phfg,gphd->fphd', attn_prob.astype(jnp.float32), qkv_parts[2])
    return mixed_rows.astype(jnp.bfloat16).reshape(frame_count, item_count, model_width)

def finish_tokens(latent_part, mixed_rows, out_weight, head_weight, gate_attn, shift_out, scale_out):
    model_width = latent_part.shape[-1]
    base_rows = latent_part.reshape(-1, model_width).astype(jnp.float32)
    branch = jnp.dot(mixed_rows.reshape(-1, model_width), out_weight, preferred_element_type=jnp.float32)
    residual = base_rows + gate_attn * branch
    final_in = modulate(residual, shift_out, scale_out)
    prediction = jnp.dot(final_in, head_weight, preferred_element_type=jnp.float32)
    return prediction.reshape(latent_part.shape[:-1] + (head_weight.shape[1],))

def block_pass(latent_block, modulation, qkv_weight, out_weight, head_weight):
    shift_attn, scale_attn, gate_attn, shift_out, scale_out = jnp.split(modulation, 5)
    normed = modulate(latent_block.astype(jnp.float32), shift_attn, scale_attn)
    mixed_rows = temporal_mix(normed, qkv_weight)
    return finish_tokens(latent_block, mixed_rows, out_weight, head_weight, gate_attn, shift_out, scale_out)

def reference(latent, text_ids, timestep, guide_num, guide_den, text_table, time_in, time_out, mod_weight, qkv_weight, out_weight, head_weight):
    time_hidden = jax.nn.silu(jnp.dot(time_features(timestep), time_in, preferred_element_type=jnp.float32)).astype(jnp.bfloat16)
    time_embed = jnp.dot(time_hidden, time_out, preferred_element_type=jnp.float32)[0]
    blocks = PIXELS // N_SEQ
    by_block = jnp.transpose(latent.reshape(FRAMES, N_SEQ, blocks, D), (1, 0, 2, 3))
    predictions = []
    for pass_index in range(2):
        ids_row = text_ids[pass_index]
        pooled = lax.optimization_barrier(jnp.sum(jnp.take(text_table, ids_row, axis=0).astype(jnp.float32), axis=0)) / jnp.sqrt(jnp.float32(TEXT))
        cond_vec = jax.nn.silu(time_embed + pooled).astype(jnp.bfloat16)
        modulation = jnp.dot(cond_vec[None, :], mod_weight, preferred_element_type=jnp.float32)[0]

        def run_block(latent_block):
            return block_pass(latent_block, modulation, qkv_weight, out_weight, head_weight)
        prediction = lax.map(run_block, by_block)
        predictions.append(jnp.transpose(prediction, (1, 0, 2, 3)).reshape(FRAMES, PIXELS, OUT_CH))
    guide_scale = guide_num[0].astype(jnp.float32) / guide_den[0].astype(jnp.float32)
    return predictions[1] + guide_scale * (predictions[0] - predictions[1])
```

```python
import functools
import math

import jax
import jax.numpy as jnp
from jax import lax
from jax.experimental import pallas as pl
from jax.experimental.pallas import tpu as pltpu
from jax.sharding import PartitionSpec as P

HEADS = 24
FREQ = 256
NORM_FLOOR = 0.1
GROUP = 128


def time_features(timestep):
    half_width = FREQ // 2
    ladder = jnp.arange(half_width, dtype=jnp.float32)
    freq_rates = jnp.exp(-math.log(10000.0) * ladder / half_width)
    angles = timestep.astype(jnp.float32)[0] * freq_rates
    return jnp.concatenate([jnp.cos(angles), jnp.sin(angles)])[None, :].astype(jnp.bfloat16)


def xor_stages(count):
    bits = count.bit_length() - 1
    assert count == 1 << bits
    stages = []
    for low in range(0, bits, 2):
        width = min(2, bits - low)
        stages.append([mask << low for mask in range(1, 1 << width)])
    return stages


def shuffle(value, mask, count):
    return lax.ppermute(value, "seq", [(i, i ^ mask) for i in range(count)])


def swap_cfg(value):
    return lax.ppermute(value, "cfg", [(0, 1), (1, 0)])


def seq_sum(value, count):
    for masks in xor_stages(count):
        value = value + sum(shuffle(value, mask, count) for mask in masks)
    return value


def seq_gather(piece, count):
    held = piece[None]
    order = [0]
    for masks in xor_stages(count):
        base, base_order = held, list(order)
        for mask in masks:
            held = jnp.concatenate([held, shuffle(base, mask, count)], axis=0)
            order += [index ^ mask for index in base_order]
    slot_of = [0] * count
    for slot, index in enumerate(order):
        slot_of[index] = slot
    wanted = jnp.array(slot_of, jnp.int32)[jnp.arange(count) ^ lax.axis_index("seq")]
    return jnp.take(held, wanted, axis=0)


def text_partial(ids_row, text_table):
    voc_rows = text_table.shape[0]
    tokens = ids_row.shape[0]
    local = (ids_row - lax.axis_index("seq") * voc_rows).reshape(8, tokens // 8)
    hits = local[:, :, None] == jnp.arange(voc_rows, dtype=jnp.int32)[None, None, :]
    counts = jnp.sum(hits.astype(jnp.float32), axis=1).astype(jnp.bfloat16)
    return jnp.sum(jnp.dot(counts, text_table, preferred_element_type=jnp.float32), axis=0)


def block_kernel(
    scale_ref, x_ref, mod_ref, wq_ref, wk_ref, wv_ref, wo_hbm, wh_ref, out_ref,
    normed, mixed, q_s, k_s, v_s, wo_s, sem,
):
    step = pl.program_id(0)
    steps = pl.num_programs(0)
    frames, items, width = x_ref.shape
    tokens = frames * items
    per_group = GROUP // frames
    groups = tokens // GROUP
    cols = wq_ref.shape[1]

    def latent_group(g):
        rows = x_ref[:, g * per_group : (g + 1) * per_group, :].astype(jnp.float32)
        return rows.reshape(GROUP, width)

    def normalize(values):
        center = values - jnp.mean(values, axis=-1, keepdims=True)
        spread = jnp.mean(center * center, axis=-1, keepdims=True)
        return center * lax.rsqrt(spread + NORM_FLOOR)

    def mod_part(c, part):
        return mod_ref[c : c + 1, part * width : (part + 1) * width]

    @pl.when(step == 0)
    def _():
        pltpu.make_async_copy(wo_hbm, wo_s, sem).start()
        for g in range(groups):
            base = normalize(latent_group(g))
            for c in range(2):
                value = base * (1.0 + mod_part(c, 1)) + mod_part(c, 0)
                normed[c * tokens + g * GROUP : c * tokens + (g + 1) * GROUP, :] = value.astype(
                    jnp.bfloat16
                )

    for w_ref, dst in ((wq_ref, q_s), (wk_ref, k_s), (wv_ref, v_s)):
        dst[...] = jnp.dot(normed[...], w_ref[...], preferred_element_type=jnp.float32).astype(
            jnp.bfloat16
        )

    row_pix = lax.broadcasted_iota(jnp.int32, (GROUP, 2 * GROUP), 0) % per_group
    col_pix = lax.broadcasted_iota(jnp.int32, (GROUP, 2 * GROUP), 1) % per_group
    same = row_pix == col_pix
    low = lax.broadcasted_iota(jnp.int32, (GROUP, 128), 1) < 64
    zero = jnp.zeros((GROUP, 128), jnp.bfloat16)
    one = jnp.ones((GROUP, 128), jnp.bfloat16)
    ones_blk = jnp.concatenate([jnp.where(low, one, zero), jnp.where(low, zero, one)], axis=0)
    rate = math.log2(math.e) / math.sqrt(64.0)

    def split_heads(value):
        return jnp.concatenate([jnp.where(low, value, zero), jnp.where(low, zero, value)], axis=0)

    for g in range(2 * groups):
        rows = slice(g * GROUP, (g + 1) * GROUP)
        for pair in range(cols // 128):
            lanes = slice(pair * 128, (pair + 1) * 128)
            keys = split_heads(k_s[rows, lanes])
            vals = jnp.concatenate([split_heads(v_s[rows, lanes]), ones_blk], axis=1)
            scores = lax.dot_general(
                q_s[rows, lanes], keys, (((1,), (1,)), ((), ())), preferred_element_type=jnp.float32
            )
            scores = jnp.where(same, scores, -jnp.inf)
            probs = []
            for h in range(2):
                part = scores[:, h * GROUP : (h + 1) * GROUP]
                top = jnp.max(part, axis=-1, keepdims=True)
                probs.append(jnp.exp2((part - top) * rate).astype(jnp.bfloat16))
            both = jnp.dot(
                jnp.concatenate(probs, axis=1), vals, preferred_element_type=jnp.float32
            )
            mixed[step, rows, lanes] = (both[:, :128] / both[:, 128:]).astype(jnp.bfloat16)

    @pl.when(step == steps - 1)
    def _():
        pltpu.make_async_copy(wo_hbm, wo_s, sem).wait()
        guide = scale_ref[0, 0]
        for g in range(groups):
            base = latent_group(g)
            preds = []
            for c in range(2):
                rows = slice(c * tokens + g * GROUP, c * tokens + (g + 1) * GROUP)
                lhs = jnp.concatenate([mixed[j, rows, :] for j in range(mixed.shape[0])], axis=1)
                branch = jnp.dot(lhs, wo_s[...], preferred_element_type=jnp.float32)
                residual = base + mod_part(c, 2) * branch
                final = normalize(residual) * (1.0 + mod_part(c, 4)) + mod_part(c, 3)
                preds.append(
                    jnp.dot(
                        final.astype(jnp.bfloat16), wh_ref[...], preferred_element_type=jnp.float32
                    )
                )
            guided = preds[1] + guide * (preds[0] - preds[1])
            out_ref[:, g * per_group : (g + 1) * per_group, :] = guided.reshape(
                frames, per_group, guided.shape[1]
            )


def run_block(guide_scale, x, mods, qkv_weight, out_weight, head_weight):
    frames, items, width = x.shape
    tokens = frames * items
    cols = 256
    steps = width // cols
    out_ch = head_weight.shape[1]
    whole = lambda shape: pl.BlockSpec(shape, lambda j: (0,) * len(shape))
    flops = 2 * 2 * tokens * width * (4 * width + out_ch)
    return pl.pallas_call(
        block_kernel,
        grid=(steps,),
        in_specs=[
            pl.BlockSpec(memory_space=pltpu.SMEM),
            whole(x.shape),
            whole(mods.shape),
            pl.BlockSpec((width, cols), lambda j: (0, j)),
            pl.BlockSpec((width, cols), lambda j: (0, j + steps)),
            pl.BlockSpec((width, cols), lambda j: (0, j + 2 * steps)),
            pl.BlockSpec(memory_space=pl.ANY),
            whole(head_weight.shape),
        ],
        out_specs=whole((frames, items, out_ch)),
        out_shape=jax.ShapeDtypeStruct((frames, items, out_ch), jnp.float32),
        scratch_shapes=[
            pltpu.VMEM((2 * tokens, width), jnp.bfloat16),
            pltpu.VMEM((steps, 2 * tokens, cols), jnp.bfloat16),
            pltpu.VMEM((2 * tokens, cols), jnp.bfloat16),
            pltpu.VMEM((2 * tokens, cols), jnp.bfloat16),
            pltpu.VMEM((2 * tokens, cols), jnp.bfloat16),
            pltpu.VMEM(out_weight.shape, jnp.bfloat16),
            pltpu.SemaphoreType.DMA,
        ],
        compiler_params=pltpu.CompilerParams(vmem_limit_bytes=40 * 1024 * 1024),
        cost_estimate=pl.CostEstimate(
            flops=flops, bytes_accessed=8 * width * width + tokens * width * 2, transcendentals=0
        ),
        name="guided_block",
    )(guide_scale, x, mods, qkv_weight, qkv_weight, qkv_weight, out_weight, head_weight)


def on_device(
    latent, text_ids, timestep, guide_num, guide_den, text_table, time_in, time_out, mod_weight,
    qkv_weight, out_weight, head_weight,
):
    frames_dev, pixels, width = latent.shape
    seq_count = lax.axis_size("seq")
    cfg_count = lax.axis_size("cfg")
    cfg = lax.axis_index("cfg")
    seq = lax.axis_index("seq")

    half = pixels // cfg_count
    items = half // seq_count
    mine = lax.dynamic_slice_in_dim(latent, cfg * half, half, 1)
    grouped = mine.reshape(frames_dev, seq_count, items, width)
    received = lax.all_to_all(grouped, "seq", split_axis=1, concat_axis=0, tiled=True)
    frames = frames_dev * seq_count
    received = received.reshape(frames, items, width)

    ids_row = text_ids[0]
    text_part = text_partial(ids_row, text_table) / jnp.sqrt(jnp.float32(ids_row.shape[0]))
    time_hidden = jax.nn.silu(
        jnp.dot(time_features(timestep), time_in, preferred_element_type=jnp.float32)
    ).astype(jnp.bfloat16)
    time_part = jnp.dot(time_hidden, time_out, preferred_element_type=jnp.float32)[0]
    mine_cols = lax.dynamic_update_slice(
        jnp.zeros_like(text_part), time_part, (seq * time_part.shape[0],)
    )
    summed = seq_sum(text_part + mine_cols, seq_count)
    cond = jax.nn.silu(summed).astype(jnp.bfloat16)[None]
    mod_mine = jnp.dot(cond, mod_weight, preferred_element_type=jnp.float32)[0]
    mod_other = swap_cfg(mod_mine)
    mod_both = jnp.where(cfg == 0, jnp.stack([mod_mine, mod_other]), jnp.stack([mod_other, mod_mine]))
    mods = seq_gather(mod_both, seq_count).transpose(1, 0, 2).reshape(2, -1)

    guide_scale = (guide_num[0].astype(jnp.float32) / guide_den[0].astype(jnp.float32)).reshape(1, 1)
    per_group = max(1, GROUP // frames)
    x = received
    if per_group % 8:
        x = received
    combined = run_block(guide_scale, x, mods, qkv_weight, out_weight, head_weight)

    out_ch = head_weight.shape[1]
    send = combined.astype(jnp.bfloat16).reshape(seq_count, frames_dev * items * out_ch)
    send = jnp.concatenate([send] * cfg_count, axis=0)
    back = lax.all_to_all(send, ("cfg", "seq"), split_axis=0, concat_axis=0, tiled=True)
    back = back.reshape(cfg_count * seq_count, frames_dev, items, out_ch).astype(jnp.float32)
    return back.transpose(1, 0, 2, 3).reshape(frames_dev, pixels, out_ch)


def solution(mesh):
    in_specs = (
        P("seq", None, None), P("cfg", None), P(), P(), P(), P("seq", None), P(), P(None, "seq"),
        P(None, "seq"), P(), P(), P(),
    )
    return jax.shard_map(
        on_device, mesh=mesh, in_specs=in_specs, out_specs=P("seq", None, None), check_vma=False
    )
```

```python
import functools
import math

import jax
import jax.numpy as jnp
from jax import lax
from jax.experimental import pallas as pl
from jax.experimental.pallas import tpu as pltpu
from jax.sharding import PartitionSpec as P

HEADS = 24
FREQ = 256
NORM_FLOOR = 0.1
GROUP = 128


def time_features(timestep):
    half_width = FREQ // 2
    ladder = jnp.arange(half_width, dtype=jnp.float32)
    freq_rates = jnp.exp(-math.log(10000.0) * ladder / half_width)
    angles = timestep.astype(jnp.float32)[0] * freq_rates
    return jnp.concatenate([jnp.cos(angles), jnp.sin(angles)])[None, :].astype(jnp.bfloat16)


def xor_stages(count):
    bits = count.bit_length() - 1
    assert count == 1 << bits
    stages = []
    for low in range(0, bits, 2):
        width = min(2, bits - low)
        stages.append([mask << low for mask in range(1, 1 << width)])
    return stages


def shuffle(value, mask, count):
    return lax.ppermute(value, "seq", [(i, i ^ mask) for i in range(count)])


def seq_sum(value, count):
    for masks in xor_stages(count):
        value = value + sum(shuffle(value, mask, count) for mask in masks)
    return value


def text_partial(ids_row, text_table):
    voc_rows = text_table.shape[0]
    tokens = ids_row.shape[0]
    local = (ids_row - lax.axis_index("seq") * voc_rows).reshape(8, tokens // 8)
    hits = local[:, :, None] == jnp.arange(voc_rows, dtype=jnp.int32)[None, None, :]
    counts = jnp.sum(hits.astype(jnp.float32), axis=1).astype(jnp.bfloat16)
    return jnp.sum(jnp.dot(counts, text_table, preferred_element_type=jnp.float32), axis=0)


def block_kernel(
    num_ref, den_ref, x_ref, mod_ref, wq_ref, wk_ref, wv_ref, wo_hbm, wh_ref, *rest, mod_cols, part
):
    if part:
        prev_ref, *rest = rest
    out_ref, mods, normed, mixed, q_s, k_s, v_s, wo_s, sem = rest
    step = pl.program_id(0)
    steps = pl.num_programs(0)
    frames, items, width = x_ref.shape
    tokens = frames * items
    per_group = GROUP // frames
    groups = tokens // GROUP
    cols = wq_ref.shape[1]

    def latent_group(g):
        rows = x_ref[:, g * per_group : (g + 1) * per_group, :].astype(jnp.float32)
        return rows.reshape(GROUP, width)

    def normalize(values):
        center = values - jnp.mean(values, axis=-1, keepdims=True)
        spread = jnp.mean(center * center, axis=-1, keepdims=True)
        return center * lax.rsqrt(spread + NORM_FLOOR)

    def mod_part(c, index):
        return mods[c : c + 1, index * width : (index + 1) * width]

    @pl.when(step == 0)
    def _():
        pltpu.make_async_copy(wo_hbm, wo_s, sem).start()
        pieces = mod_ref.shape[0] // 2
        for c in range(2):
            for piece in range(pieces):
                for row in range(mod_ref.shape[1]):
                    size = min(128, mod_cols - row * 128)
                    start = piece * mod_cols + row * 128
                    mods[c : c + 1, start : start + size] = mod_ref[
                        c * pieces + piece, row : row + 1, :size
                    ]
        for g in range(groups):
            base = normalize(latent_group(g))
            for c in range(2):
                value = base * (1.0 + mod_part(c, 1)) + mod_part(c, 0)
                normed[c * tokens + g * GROUP : c * tokens + (g + 1) * GROUP, :] = value.astype(
                    jnp.bfloat16
                )

    for w_ref, dst in ((wq_ref, q_s), (wk_ref, k_s), (wv_ref, v_s)):
        dst[...] = jnp.dot(normed[...], w_ref[...], preferred_element_type=jnp.float32).astype(
            jnp.bfloat16
        )

    def attend():
        row_pix = lax.broadcasted_iota(jnp.int32, (GROUP, GROUP), 0) % per_group
        col_pix = lax.broadcasted_iota(jnp.int32, (GROUP, GROUP), 1) % per_group
        same = row_pix == col_pix
        low = lax.broadcasted_iota(jnp.int32, (GROUP, 128), 1) < 64
        zero = jnp.zeros((GROUP, 128), jnp.bfloat16)
        one = jnp.ones((GROUP, 128), jnp.bfloat16)
        ones_blk = jnp.concatenate([jnp.where(low, one, zero), jnp.where(low, zero, one)], axis=0)
        rate = math.log2(math.e) / math.sqrt(64.0)

        def split_heads(value):
            return jnp.concatenate(
                [jnp.where(low, value, zero), jnp.where(low, zero, value)], axis=0
            )

        def unit(rows, lanes):
            keys = split_heads(k_s[rows, lanes])
            vals = jnp.concatenate([split_heads(v_s[rows, lanes]), ones_blk], axis=1)
            scores = lax.dot_general(
                q_s[rows, lanes], keys, (((1,), (1,)), ((), ())), preferred_element_type=jnp.float32
            )
            probs = []
            for h in range(2):
                part = jnp.where(same, scores[:, h * GROUP : (h + 1) * GROUP], -jnp.inf)
                top = jnp.max(part, axis=-1, keepdims=True)
                probs.append(jnp.exp2((part - top) * rate).astype(jnp.bfloat16))
            both = jnp.dot(
                jnp.concatenate(probs, axis=1), vals, preferred_element_type=jnp.float32
            )
            mixed[step, rows, lanes] = (both[:, :128] / both[:, 128:]).astype(jnp.bfloat16)

        for g in range(2 * groups):
            for pair in range(cols // 128):
                unit(slice(g * GROUP, (g + 1) * GROUP), slice(pair * 128, (pair + 1) * 128))

    pl.when(step >= 0)(attend)

    @pl.when(step == steps - 1)
    def _():
        pltpu.make_async_copy(wo_hbm, wo_s, sem).wait()
        guide = jnp.full((1, 1), num_ref[0].astype(jnp.float32)) / jnp.full(
            (1, 1), den_ref[0].astype(jnp.float32)
        )
        preds = []
        for c in range(2):
            rows = slice(c * tokens, (c + 1) * tokens)
            lhs = jnp.concatenate([mixed[j, rows, :] for j in range(mixed.shape[0])], axis=1)
            branch = jnp.dot(lhs, wo_s[...], preferred_element_type=jnp.float32)
            base = jnp.concatenate([latent_group(g) for g in range(groups)], axis=0)
            residual = base + mod_part(c, 2) * branch
            final = normalize(residual) * (1.0 + mod_part(c, 4)) + mod_part(c, 3)
            preds.append(
                lax.dot_general(
                    final.astype(jnp.bfloat16), wh_ref[...], (((1,), (1,)), ((), ())),
                    preferred_element_type=jnp.float32,
                )
            )
        guided = preds[1] + guide * (preds[0] - preds[1])
        wide = jnp.concatenate([guided[: tokens // 2], guided[tokens // 2 :]], axis=1)
        held = items // 2
        for g in range(groups // 2):
            block = wide[g * GROUP : (g + 1) * GROUP].reshape(frames, per_group, wide.shape[1])
            block = block.astype(out_ref.dtype)
            first = part * held + g * per_group
            for copy in range(out_ref.shape[0]):
                out_ref[copy, :, first : first + per_group, :] = block
        if part:
            out_ref[:, :, : part * held, :] = prev_ref[...]


def run_block(
    guide_num, guide_den, x, mods, mod_cols, qkv_weight, out_weight, head_rows, copies, prev
):
    frames, items, width = x.shape
    tokens = frames * items
    cols = 256
    steps = width // cols
    out_ch = head_rows.shape[0]
    part = 0 if prev is None else prev.shape[2] // (items // 2)
    out_dims = (copies, frames, (part + 1) * (items // 2), 2 * out_ch)
    whole = lambda shape: pl.BlockSpec(shape, lambda j: (0,) * len(shape))
    flops = 2 * 2 * tokens * width * (4 * width + out_ch)
    more = [] if prev is None else [prev]
    return pl.pallas_call(
        functools.partial(block_kernel, mod_cols=mod_cols, part=part),
        grid=(steps,),
        in_specs=[
            pl.BlockSpec(memory_space=pltpu.SMEM),
            pl.BlockSpec(memory_space=pltpu.SMEM),
            whole(x.shape),
            whole(mods.shape),
            pl.BlockSpec((width, cols), lambda j: (0, j)),
            pl.BlockSpec((width, cols), lambda j: (0, j + steps)),
            pl.BlockSpec((width, cols), lambda j: (0, j + 2 * steps)),
            pl.BlockSpec(memory_space=pltpu.HBM),
            whole(head_rows.shape),
            *(whole(extra.shape) for extra in more),
        ],
        out_specs=whole(out_dims),
        out_shape=jax.ShapeDtypeStruct(out_dims, jnp.bfloat16),
        scratch_shapes=[
            pltpu.VMEM((2, 5 * width), jnp.float32),
            pltpu.VMEM((2 * tokens, width), jnp.bfloat16),
            pltpu.VMEM((steps, 2 * tokens, cols), jnp.bfloat16),
            pltpu.VMEM((2 * tokens, cols), jnp.bfloat16),
            pltpu.VMEM((2 * tokens, cols), jnp.bfloat16),
            pltpu.VMEM((2 * tokens, cols), jnp.bfloat16),
            pltpu.VMEM(out_weight.shape, jnp.bfloat16),
            pltpu.SemaphoreType.DMA,
        ],
        compiler_params=pltpu.CompilerParams(vmem_limit_bytes=58 * 1024 * 1024),
        cost_estimate=pl.CostEstimate(
            flops=flops, bytes_accessed=8 * width * width + tokens * width * 2, transcendentals=0
        ),
        name="guided_block",
    )(
        guide_num, guide_den, x, mods, qkv_weight, qkv_weight, qkv_weight, out_weight, head_rows, *more
    )


def order_kernel(x_ref, out_ref, *, portions):
    devices, _, rows, lanes = x_ref.shape
    run_len = rows // portions
    out_ch = lanes // 2
    span = devices * run_len
    for p in range(portions):
        block = x_ref[:, 0, p * run_len : (p + 1) * run_len, :].astype(jnp.float32)
        turned = block.reshape(span, lanes).T
        for h in range(2):
            out_ref[0, :, (2 * p + h) * span : (2 * p + h + 1) * span] = turned[
                h * out_ch : (h + 1) * out_ch
            ]


def in_order(back, portions):
    devices, frames_dev, rows, lanes = back.shape
    run_len = rows // portions
    pixels = devices * rows * 2
    out_ch = lanes // 2
    if frames_dev > 1 or run_len % 8:
        parts = back.reshape(devices, frames_dev, portions, run_len, 2, out_ch)
        parts = parts.transpose(1, 2, 4, 0, 3, 5).reshape(frames_dev, pixels, out_ch)
        return parts.astype(jnp.float32)
    turned = pl.pallas_call(
        functools.partial(order_kernel, portions=portions),
        out_shape=jax.ShapeDtypeStruct((1, out_ch, pixels), jnp.float32),
        name="in_order",
    )(back)
    return turned.transpose(0, 2, 1)


def on_device(
    latent, text_ids, timestep, guide_num, guide_den, text_table, time_in, time_out, mod_weight,
    qkv_weight, out_weight, head_weight,
):
    frames_dev, pixels, width = latent.shape
    seq_count = lax.axis_size("seq")
    cfg_count = lax.axis_size("cfg")
    cfg = lax.axis_index("cfg")
    seq = lax.axis_index("seq")

    half = pixels // cfg_count
    items = half // seq_count
    frames = frames_dev * seq_count
    portions = 2
    some = items // portions
    run_len = some // 2
    devices = cfg_count * seq_count
    mine = latent.reshape(frames_dev, portions, 2, cfg_count, seq_count, run_len, width)
    mine = lax.dynamic_index_in_dim(mine, cfg, 3, keepdims=False)
    mine = mine.transpose(0, 1, 3, 2, 4, 5).reshape(
        frames_dev, portions, seq_count, some, width
    )

    def exchange(portion):
        got = lax.all_to_all(portion, "seq", split_axis=1, concat_axis=0, tiled=True)
        return got.reshape(frames, some, width)

    received = exchange(mine[:, 0])

    ids_row = text_ids[0]
    text_part = text_partial(ids_row, text_table) / jnp.sqrt(jnp.float32(ids_row.shape[0]))
    time_hidden = jax.nn.silu(
        jnp.dot(time_features(timestep), time_in, preferred_element_type=jnp.float32)
    ).astype(jnp.bfloat16)
    time_part = jnp.dot(time_hidden, time_out, preferred_element_type=jnp.float32)[0]
    mine_cols = lax.dynamic_update_slice(
        jnp.zeros_like(text_part), time_part, (seq * time_part.shape[0],)
    )
    summed = seq_sum(text_part + mine_cols, seq_count)
    cond = jax.nn.silu(summed).astype(jnp.bfloat16)[None]
    mod_mine = jnp.dot(cond, mod_weight, preferred_element_type=jnp.float32)
    mod_mine, received = lax.optimization_barrier((mod_mine, received))
    mod_cols = mod_mine.shape[1]
    lines = -(-mod_cols // 128)
    piece = jnp.pad(mod_mine[0], (0, lines * 128 - mod_cols)).reshape(1, lines, 128)
    mods = lax.all_to_all(
        jnp.broadcast_to(piece, (devices, lines, 128)), ("cfg", "seq"),
        split_axis=0, concat_axis=0, tiled=True,
    )
    mods, rest = lax.optimization_barrier((mods, mine[:, 1]))
    run = lambda x, prev: run_block(
        guide_num, guide_den, x, mods, mod_cols, qkv_weight, out_weight, head_weight.T, cfg_count, prev
    )
    later = exchange(rest)
    combined = run(later, run(received, None))
    out_ch = head_weight.shape[1]
    send = combined.reshape(devices, frames_dev, items // 2, 2 * out_ch)
    back = lax.all_to_all(send, ("cfg", "seq"), split_axis=0, concat_axis=0, tiled=True)
    return in_order(back, portions)


def solution(mesh):
    in_specs = (
        P("seq", None, None), P("cfg", None), P(), P(), P(), P("seq", None), P(), P(None, "seq"),
        P(None, "seq"), P(), P(), P(),
    )
    return jax.shard_map(
        on_device, mesh=mesh, in_specs=in_specs, out_specs=P("seq", None, None), check_vma=False
    )
```

```python
import functools
import math

import jax
import jax.numpy as jnp
from jax import lax
from jax.experimental import pallas as pl
from jax.experimental.pallas import tpu as pltpu
from jax.sharding import PartitionSpec as P

HEADS = 24
FREQ = 256
NORM_FLOOR = 0.1
GROUP = 128


def time_features(timestep):
    half_width = FREQ // 2
    ladder = jnp.arange(half_width, dtype=jnp.float32)
    freq_rates = jnp.exp(-math.log(10000.0) * ladder / half_width)
    angles = timestep.astype(jnp.float32)[0] * freq_rates
    return jnp.concatenate([jnp.cos(angles), jnp.sin(angles)])[None, :].astype(jnp.bfloat16)


def xor_stages(count):
    bits = count.bit_length() - 1
    assert count == 1 << bits
    stages = []
    for low in range(0, bits, 2):
        width = min(2, bits - low)
        stages.append([mask << low for mask in range(1, 1 << width)])
    return stages


def shuffle(value, mask, count):
    return lax.ppermute(value, "seq", [(i, i ^ mask) for i in range(count)])


def seq_sum(value, count):
    for masks in xor_stages(count):
        value = value + sum(shuffle(value, mask, count) for mask in masks)
    return value


def text_partial(ids_row, text_table):
    voc_rows = text_table.shape[0]
    tokens = ids_row.shape[0]
    local = (ids_row - lax.axis_index("seq") * voc_rows).reshape(8, tokens // 8)
    hits = local[:, :, None] == jnp.arange(voc_rows, dtype=jnp.int32)[None, None, :]
    counts = jnp.sum(hits.astype(jnp.float32), axis=1).astype(jnp.bfloat16)
    return jnp.sum(jnp.dot(counts, text_table, preferred_element_type=jnp.float32), axis=0)


def text_kernel(
    ids_ref, freq_ref, time_in_ref, time_out_ref, table_hbm, out_ref, table, spread, sems
):
    voc_rows, width = table_hbm.shape
    chunk = 256
    chunks = table.shape[0] // chunk
    tokens = ids_ref.shape[1]
    seq = lax.axis_index("seq")

    def fetch(index):
        rows = min(chunk, voc_rows - index * chunk)
        at = pl.ds(index * chunk, rows)
        return pltpu.make_async_copy(table_hbm.at[at, :], table.at[at, :], sems.at[index])

    for index in range(chunks):
        fetch(index).start()
    pad = table.shape[0] - voc_rows
    if pad:
        table[voc_rows:, :] = jnp.zeros((pad, width), table.dtype)

    group = tokens // 8
    local = jnp.concatenate(
        [ids_ref[:, row * group : (row + 1) * group] for row in range(8)], axis=0
    ) - seq * voc_rows
    lane = lax.broadcasted_iota(jnp.int32, (8, table.shape[0]), 1)
    counts = jnp.zeros((8, table.shape[0]), jnp.float32)
    for token in range(group):
        counts = counts + jnp.where(local[:, token : token + 1] == lane, 1.0, 0.0)
    counts = counts.astype(jnp.bfloat16)
    feats = jnp.broadcast_to(freq_ref[...], (8, freq_ref.shape[1]))
    hidden = jnp.dot(feats, time_in_ref[...], preferred_element_type=jnp.float32)
    hidden = (hidden / (1.0 + jnp.exp(-hidden))).astype(jnp.bfloat16)
    embed = lax.dot_general(
        hidden, time_out_ref[...], (((1,), (1,)), ((), ())), preferred_element_type=jnp.float32
    )[:1]
    mine = embed.shape[1]
    for piece in range(width // mine):
        spread[:, piece * mine : (piece + 1) * mine] = embed
    owner = lax.broadcasted_iota(jnp.int32, (1, width), 1) // mine
    total = jnp.zeros((8, width), jnp.float32)

    for index in range(chunks):
        fetch(index).wait()
        rows = slice(index * chunk, (index + 1) * chunk)
        total = total + jnp.dot(
            counts[:, rows], table[rows, :], preferred_element_type=jnp.float32
        )
    text = jnp.sum(total, axis=0, keepdims=True) / math.sqrt(tokens)
    out_ref[...] = text + jnp.where(owner == seq, spread[...], 0.0)


def conditioning_part(text_ids, freqs, text_table, time_in, time_out):
    voc_rows, width = text_table.shape
    tokens = text_ids.shape[1]
    if voc_rows % 8 or tokens % 64:
        text = text_partial(text_ids[0], text_table) / jnp.sqrt(jnp.float32(tokens))
        hidden = jax.nn.silu(jnp.dot(freqs, time_in, preferred_element_type=jnp.float32))
        embed = jnp.dot(
            hidden.astype(jnp.bfloat16), time_out, preferred_element_type=jnp.float32
        )[0]
        start = lax.axis_index("seq") * embed.shape[0]
        return (text + lax.dynamic_update_slice(jnp.zeros_like(text), embed, (start,)))[None]
    chunks = -(-voc_rows // 256)
    vmem = pl.BlockSpec(memory_space=pltpu.VMEM)
    out = pl.pallas_call(
        text_kernel,
        in_specs=[vmem] * 4 + [pl.BlockSpec(memory_space=pltpu.HBM)],
        out_specs=vmem,
        out_shape=jax.ShapeDtypeStruct((1, width), jnp.float32),
        scratch_shapes=[
            pltpu.VMEM((chunks * 256, width), text_table.dtype),
            pltpu.VMEM((1, width), jnp.float32),
            pltpu.SemaphoreType.DMA((chunks,)),
        ],
        cost_estimate=pl.CostEstimate(
            flops=2 * 8 * voc_rows * width, bytes_accessed=2 * voc_rows * width, transcendentals=0
        ),
        name="text_part",
    )(text_ids, freqs, time_in, time_out.T, text_table)
    return out


def portion_kernel(x_hbm, *rest):
    outs, (held, in_sem, out_sem) = rest[:-3], rest[-3:]
    cfg_count = x_hbm.shape[1]
    run_len = x_hbm.shape[3]
    cfg = lax.axis_index("cfg")
    get = [
        pltpu.make_async_copy(x_hbm.at[index, cfg], held.at[index], in_sem.at[index])
        for index in range(held.shape[0])
    ]
    put = [
        pltpu.make_async_copy(
            held.at[index],
            outs[index // 2].at[:, (index % 2) * run_len : (index % 2 + 1) * run_len, :],
            out_sem.at[index],
        )
        for index in range(held.shape[0])
    ]
    for copy in get:
        copy.start()
    for index, copy in enumerate(put):
        get[index].wait()
        copy.start()
    for copy in put:
        copy.wait()


def portions_to_send(latent, portions, seq_count, cfg_count):
    frames_dev, pixels, width = latent.shape
    run_len = pixels // (portions * 2 * cfg_count * seq_count)
    if frames_dev > 1 or run_len % 8:
        mine = latent.reshape(frames_dev, portions, 2, cfg_count, seq_count, run_len, width)
        mine = lax.dynamic_index_in_dim(mine, lax.axis_index("cfg"), 3, keepdims=False)
        mine = mine.transpose(0, 1, 3, 2, 4, 5).reshape(
            frames_dev, portions, seq_count, 2 * run_len, width
        )
        return [mine[:, index] for index in range(portions)]
    view = latent.reshape(portions * 2, cfg_count, seq_count, run_len, width)
    dims = (seq_count, 2 * run_len, width)
    hbm = pl.BlockSpec(memory_space=pltpu.HBM)
    outs = pl.pallas_call(
        portion_kernel,
        in_specs=[hbm],
        out_specs=[hbm] * portions,
        out_shape=[jax.ShapeDtypeStruct(dims, latent.dtype)] * portions,
        scratch_shapes=[
            pltpu.VMEM((portions * 2, seq_count, run_len, width), latent.dtype),
            pltpu.SemaphoreType.DMA((portions * 2,)),
            pltpu.SemaphoreType.DMA((portions * 2,)),
        ],
        name="portions",
    )(view)
    return [out[None] for out in outs]


def block_kernel(
    num_ref, den_ref, x_ref, mod_ref, w_hbm, wo_hbm, wh_ref, *rest, mod_cols, part
):
    if part:
        prev_ref, *rest = rest
    out_ref, mods, normed, mixed, qkv_s, w_s, wo_s, w_sem, sem = rest
    cols = w_s.shape[2] // 3
    q_s, k_s, v_s = (qkv_s.at[:, index * cols : (index + 1) * cols] for index in range(3))
    step = pl.program_id(0)
    steps = pl.num_programs(0)
    frames, items, width = x_ref.shape
    tokens = frames * items
    per_group = GROUP // frames
    groups = tokens // GROUP

    def weight_copy(index, block):
        return pltpu.make_async_copy(
            w_hbm.at[:, pl.ds(pl.multiple_of(index * width + block * cols, cols), cols)],
            w_s.at[block, :, index * cols : (index + 1) * cols],
            w_sem.at[index, block],
        )

    def latent_group(g):
        rows = x_ref[:, g * per_group : (g + 1) * per_group, :].astype(jnp.float32)
        return rows.reshape(GROUP, width)

    def normalize(values):
        center = values - jnp.mean(values, axis=-1, keepdims=True)
        spread = jnp.mean(center * center, axis=-1, keepdims=True)
        return center * lax.rsqrt(spread + NORM_FLOOR)

    def mod_part(c, index):
        return mods[c : c + 1, index * width : (index + 1) * width]

    @pl.when(step == 0)
    def _():
        for block in range(w_s.shape[0]):
            for index in range(3):
                weight_copy(index, block).start()
        pltpu.make_async_copy(wo_hbm, wo_s, sem).start()
        pieces = mod_ref.shape[0] // 2
        for c in range(2):
            for piece in range(pieces):
                for row in range(mod_ref.shape[1]):
                    size = min(128, mod_cols - row * 128)
                    start = piece * mod_cols + row * 128
                    mods[c : c + 1, start : start + size] = mod_ref[
                        c * pieces + piece, row : row + 1, :size
                    ]
        for g in range(groups):
            base = normalize(latent_group(g))
            for c in range(2):
                value = base * (1.0 + mod_part(c, 1)) + mod_part(c, 0)
                normed[c * tokens + g * GROUP : c * tokens + (g + 1) * GROUP, :] = value.astype(
                    jnp.bfloat16
                )

    for index in range(3):
        weight_copy(index, step).wait()
    qkv_s[...] = jnp.dot(normed[...], w_s[step], preferred_element_type=jnp.float32).astype(
        jnp.bfloat16
    )

    def attend():
        row_pix = lax.broadcasted_iota(jnp.int32, (GROUP, GROUP), 0) % per_group
        col_pix = lax.broadcasted_iota(jnp.int32, (GROUP, GROUP), 1) % per_group
        same = row_pix == col_pix
        low = lax.broadcasted_iota(jnp.int32, (GROUP, 128), 1) < 64
        zero = jnp.zeros((GROUP, 128), jnp.bfloat16)
        one = jnp.ones((GROUP, 128), jnp.bfloat16)
        ones_blk = jnp.concatenate([jnp.where(low, one, zero), jnp.where(low, zero, one)], axis=0)
        rate = math.log2(math.e) / math.sqrt(64.0)

        def split_heads(value):
            return jnp.concatenate(
                [jnp.where(low, value, zero), jnp.where(low, zero, value)], axis=0
            )

        def unit(rows, lanes):
            keys = split_heads(k_s[rows, lanes])
            vals = jnp.concatenate([split_heads(v_s[rows, lanes]), ones_blk], axis=1)
            scores = lax.dot_general(
                q_s[rows, lanes], keys, (((1,), (1,)), ((), ())), preferred_element_type=jnp.float32
            )
            probs = []
            for h in range(2):
                part = jnp.where(same, scores[:, h * GROUP : (h + 1) * GROUP], -jnp.inf)
                top = jnp.max(part, axis=-1, keepdims=True)
                probs.append(jnp.exp2((part - top) * rate).astype(jnp.bfloat16))
            both = jnp.dot(
                jnp.concatenate(probs, axis=1), vals, preferred_element_type=jnp.float32
            )
            mixed[step, rows, lanes] = (both[:, :128] / both[:, 128:]).astype(jnp.bfloat16)

        for g in range(2 * groups):
            for pair in range(cols // 128):
                unit(slice(g * GROUP, (g + 1) * GROUP), slice(pair * 128, (pair + 1) * 128))

    pl.when(step >= 0)(attend)

    @pl.when(step == steps - 1)
    def _():
        pltpu.make_async_copy(wo_hbm, wo_s, sem).wait()
        guide = num_ref[...].astype(jnp.float32) / den_ref[...].astype(jnp.float32)
        preds = []
        lhs = jnp.concatenate([mixed[j] for j in range(mixed.shape[0])], axis=1)
        branch = jnp.dot(lhs, wo_s[...], preferred_element_type=jnp.float32)
        for c in range(2):
            base = jnp.concatenate([latent_group(g) for g in range(groups)], axis=0)
            residual = base + mod_part(c, 2) * branch[c * tokens : (c + 1) * tokens]
            final = normalize(residual) * (1.0 + mod_part(c, 4)) + mod_part(c, 3)
            preds.append(
                lax.dot_general(
                    final.astype(jnp.bfloat16), wh_ref[...], (((1,), (1,)), ((), ())),
                    preferred_element_type=jnp.float32,
                )
            )
        guided = preds[1] + guide * (preds[0] - preds[1])
        wide = jnp.concatenate([guided[: tokens // 2], guided[tokens // 2 :]], axis=1)
        held = items // 2
        for g in range(groups // 2):
            block = wide[g * GROUP : (g + 1) * GROUP].reshape(frames, per_group, wide.shape[1])
            block = block.astype(out_ref.dtype)
            first = part * held + g * per_group
            for copy in range(out_ref.shape[0]):
                out_ref[copy, :, first : first + per_group, :] = block
        if part:
            out_ref[:, :, : part * held, :] = prev_ref[...]


def run_block(
    guide_num, guide_den, x, mods, mod_cols, qkv_weight, out_weight, head_rows, copies, prev
):
    frames, items, width = x.shape
    tokens = frames * items
    cols = 512 if width % 512 == 0 else 256
    steps = width // cols
    out_ch = head_rows.shape[0]
    part = 0 if prev is None else prev.shape[2] // (items // 2)
    out_dims = (copies, frames, (part + 1) * (items // 2), 2 * out_ch)
    whole = lambda shape: pl.BlockSpec(shape, lambda j: (0,) * len(shape))
    flops = 2 * 2 * tokens * width * (4 * width + out_ch)
    more = [] if prev is None else [prev]
    return pl.pallas_call(
        functools.partial(block_kernel, mod_cols=mod_cols, part=part),
        grid=(steps,),
        in_specs=[
            whole((1, 1)),
            whole((1, 1)),
            whole(x.shape),
            whole(mods.shape),
            pl.BlockSpec(memory_space=pltpu.HBM),
            pl.BlockSpec(memory_space=pltpu.HBM),
            whole(head_rows.shape),
            *(whole(extra.shape) for extra in more),
        ],
        out_specs=whole(out_dims),
        out_shape=jax.ShapeDtypeStruct(out_dims, jnp.bfloat16),
        scratch_shapes=[
            pltpu.VMEM((2, 5 * width), jnp.float32),
            pltpu.VMEM((2 * tokens, width), jnp.bfloat16),
            pltpu.VMEM((steps, 2 * tokens, cols), jnp.bfloat16),
            pltpu.VMEM((2 * tokens, 3 * cols), jnp.bfloat16),
            pltpu.VMEM((steps, width, 3 * cols), jnp.bfloat16),
            pltpu.VMEM(out_weight.shape, jnp.bfloat16),
            pltpu.SemaphoreType.DMA((3, steps)),
            pltpu.SemaphoreType.DMA,
        ],
        compiler_params=pltpu.CompilerParams(vmem_limit_bytes=66_500_000),
        cost_estimate=pl.CostEstimate(
            flops=flops, bytes_accessed=8 * width * width + tokens * width * 2, transcendentals=0
        ),
        name="guided_block",
    )(
        guide_num.reshape(1, 1), guide_den.reshape(1, 1), x, mods, qkv_weight, out_weight, head_rows,
        *more
    )


def order_kernel(x_ref, out_ref, *, portions):
    devices, _, rows, lanes = x_ref.shape
    run_len = rows // portions
    out_ch = lanes // 2
    span = devices * run_len
    for p in range(portions):
        block = x_ref[:, 0, p * run_len : (p + 1) * run_len, :].astype(jnp.float32)
        turned = block.reshape(span, lanes).T
        for h in range(2):
            out_ref[0, :, (2 * p + h) * span : (2 * p + h + 1) * span] = turned[
                h * out_ch : (h + 1) * out_ch
            ]


def in_order(back, portions):
    devices, frames_dev, rows, lanes = back.shape
    run_len = rows // portions
    pixels = devices * rows * 2
    out_ch = lanes // 2
    if frames_dev > 1 or run_len % 8:
        parts = back.reshape(devices, frames_dev, portions, run_len, 2, out_ch)
        parts = parts.transpose(1, 2, 4, 0, 3, 5).reshape(frames_dev, pixels, out_ch)
        return parts.astype(jnp.float32)
    turned = pl.pallas_call(
        functools.partial(order_kernel, portions=portions),
        out_shape=jax.ShapeDtypeStruct((1, out_ch, pixels), jnp.float32),
        name="in_order",
    )(back)
    return turned.transpose(0, 2, 1)


def on_device(
    latent, text_ids, timestep, guide_num, guide_den, text_table, time_in, time_out, mod_weight,
    qkv_weight, out_weight, head_weight,
):
    frames_dev, pixels, width = latent.shape
    seq_count = lax.axis_size("seq")
    cfg_count = lax.axis_size("cfg")
    half = pixels // cfg_count
    items = half // seq_count
    frames = frames_dev * seq_count
    portions = 2
    some = items // portions
    devices = cfg_count * seq_count
    mine = portions_to_send(latent, portions, seq_count, cfg_count)

    def exchange(portion):
        got = lax.all_to_all(portion, "seq", split_axis=1, concat_axis=0, tiled=True)
        return got.reshape(frames, some, width)

    received = exchange(mine[0])

    part = conditioning_part(text_ids, time_features(timestep), text_table, time_in, time_out)
    summed = seq_sum(part, seq_count)
    cond = jax.nn.silu(summed).astype(jnp.bfloat16)
    mod_mine = jnp.dot(cond, mod_weight, preferred_element_type=jnp.float32)
    mod_mine, received = lax.optimization_barrier((mod_mine, received))
    mod_cols = mod_mine.shape[1]
    lines = -(-mod_cols // 128)
    piece = jnp.pad(mod_mine[0], (0, lines * 128 - mod_cols)).reshape(1, lines, 128)
    mods = lax.all_to_all(
        jnp.broadcast_to(piece, (devices, lines, 128)), ("cfg", "seq"),
        split_axis=0, concat_axis=0, tiled=True,
    )
    mods, rest = lax.optimization_barrier((mods, mine[1]))
    run = lambda x, prev: run_block(
        guide_num, guide_den, x, mods, mod_cols, qkv_weight, out_weight, head_weight.T, cfg_count, prev
    )
    later = exchange(rest)
    combined = run(later, run(received, None))
    out_ch = head_weight.shape[1]
    send = combined.reshape(devices, frames_dev, items // 2, 2 * out_ch)
    back = lax.all_to_all(send, ("cfg", "seq"), split_axis=0, concat_axis=0, tiled=True)
    return in_order(back, portions)


def solution(mesh):
    in_specs = (
        P("seq", None, None), P("cfg", None), P(), P(), P(), P("seq", None), P(), P(None, "seq"),
        P(None, "seq"), P(), P(), P(),
    )
    return jax.shard_map(
        on_device, mesh=mesh, in_specs=in_specs, out_specs=P("seq", None, None), check_vma=False
    )
```

```python
import functools
import math

import jax
import jax.numpy as jnp
from jax import lax
from jax.experimental import pallas as pl
from jax.experimental.pallas import tpu as pltpu
from jax.sharding import PartitionSpec as P

HEADS = 24
FREQ = 256
NORM_FLOOR = 0.1
GROUP = 128


def time_features(timestep):
    half_width = FREQ // 2
    ladder = jnp.arange(half_width, dtype=jnp.float32)
    freq_rates = jnp.exp(-math.log(10000.0) * ladder / half_width)
    angles = timestep.astype(jnp.float32)[0] * freq_rates
    return jnp.concatenate([jnp.cos(angles), jnp.sin(angles)])[None, :].astype(jnp.bfloat16)


def xor_stages(count):
    bits = count.bit_length() - 1
    assert count == 1 << bits
    stages = []
    for low in range(0, bits, 2):
        width = min(2, bits - low)
        stages.append([mask << low for mask in range(1, 1 << width)])
    return stages


def shuffle(value, mask, count):
    return lax.ppermute(value, "seq", [(i, i ^ mask) for i in range(count)])


def seq_sum(value, count):
    for masks in xor_stages(count):
        value = value + sum(shuffle(value, mask, count) for mask in masks)
    return value


def text_partial(ids_row, text_table):
    voc_rows = text_table.shape[0]
    tokens = ids_row.shape[0]
    local = (ids_row - lax.axis_index("seq") * voc_rows).reshape(8, tokens // 8)
    hits = local[:, :, None] == jnp.arange(voc_rows, dtype=jnp.int32)[None, None, :]
    counts = jnp.sum(hits.astype(jnp.float32), axis=1).astype(jnp.bfloat16)
    return jnp.sum(jnp.dot(counts, text_table, preferred_element_type=jnp.float32), axis=0)


def text_kernel(
    ids_ref, freq_ref, time_in_ref, time_out_ref, table_hbm, out_ref, table, spread, sems
):
    voc_rows, width = table_hbm.shape
    chunk = 256
    chunks = table.shape[0] // chunk
    tokens = ids_ref.shape[1]
    seq = lax.axis_index("seq")

    def fetch(index):
        rows = min(chunk, voc_rows - index * chunk)
        at = pl.ds(index * chunk, rows)
        return pltpu.make_async_copy(table_hbm.at[at, :], table.at[at, :], sems.at[index])

    for index in range(chunks):
        fetch(index).start()
    pad = table.shape[0] - voc_rows
    if pad:
        table[voc_rows:, :] = jnp.zeros((pad, width), table.dtype)

    group = tokens // 8
    local = jnp.concatenate(
        [ids_ref[:, row * group : (row + 1) * group] for row in range(8)], axis=0
    ) - seq * voc_rows
    lane = lax.broadcasted_iota(jnp.int32, (8, table.shape[0]), 1)
    counts = jnp.zeros((8, table.shape[0]), jnp.float32)
    for token in range(group):
        counts = counts + jnp.where(local[:, token : token + 1] == lane, 1.0, 0.0)
    counts = counts.astype(jnp.bfloat16)
    feats = jnp.broadcast_to(freq_ref[...], (8, freq_ref.shape[1]))
    hidden = jnp.dot(feats, time_in_ref[...], preferred_element_type=jnp.float32)
    hidden = (hidden / (1.0 + jnp.exp(-hidden))).astype(jnp.bfloat16)
    embed = lax.dot_general(
        hidden, time_out_ref[...], (((1,), (1,)), ((), ())), preferred_element_type=jnp.float32
    )[:1]
    mine = embed.shape[1]
    for piece in range(width // mine):
        spread[:, piece * mine : (piece + 1) * mine] = embed
    owner = lax.broadcasted_iota(jnp.int32, (1, width), 1) // mine
    total = jnp.zeros((8, width), jnp.float32)

    for index in range(chunks):
        fetch(index).wait()
        rows = slice(index * chunk, (index + 1) * chunk)
        total = total + jnp.dot(
            counts[:, rows], table[rows, :], preferred_element_type=jnp.float32
        )
    text = jnp.sum(total, axis=0, keepdims=True) / math.sqrt(tokens)
    out_ref[...] = text + jnp.where(owner == seq, spread[...], 0.0)


def conditioning_part(text_ids, freqs, text_table, time_in, time_out):
    voc_rows, width = text_table.shape
    tokens = text_ids.shape[1]
    if voc_rows % 8 or tokens % 64:
        text = text_partial(text_ids[0], text_table) / jnp.sqrt(jnp.float32(tokens))
        hidden = jax.nn.silu(jnp.dot(freqs, time_in, preferred_element_type=jnp.float32))
        embed = jnp.dot(
            hidden.astype(jnp.bfloat16), time_out, preferred_element_type=jnp.float32
        )[0]
        start = lax.axis_index("seq") * embed.shape[0]
        return (text + lax.dynamic_update_slice(jnp.zeros_like(text), embed, (start,)))[None]
    chunks = -(-voc_rows // 256)
    vmem = pl.BlockSpec(memory_space=pltpu.VMEM)
    out = pl.pallas_call(
        text_kernel,
        in_specs=[vmem] * 4 + [pl.BlockSpec(memory_space=pltpu.HBM)],
        out_specs=vmem,
        out_shape=jax.ShapeDtypeStruct((1, width), jnp.float32),
        scratch_shapes=[
            pltpu.VMEM((chunks * 256, width), text_table.dtype),
            pltpu.VMEM((1, width), jnp.float32),
            pltpu.SemaphoreType.DMA((chunks,)),
        ],
        cost_estimate=pl.CostEstimate(
            flops=2 * 8 * voc_rows * width, bytes_accessed=2 * voc_rows * width, transcendentals=0
        ),
        name="text_part",
    )(text_ids, freqs, time_in, time_out.T, text_table)
    return out


def portion_kernel(x_hbm, *rest):
    outs, (held, in_sem, out_sem) = rest[:-3], rest[-3:]
    cfg_count = x_hbm.shape[1]
    run_len = x_hbm.shape[3]
    cfg = lax.axis_index("cfg")
    get = [
        pltpu.make_async_copy(x_hbm.at[index, cfg], held.at[index], in_sem.at[index])
        for index in range(held.shape[0])
    ]
    put = [
        pltpu.make_async_copy(
            held.at[index],
            outs[index // 2].at[:, (index % 2) * run_len : (index % 2 + 1) * run_len, :],
            out_sem.at[index],
        )
        for index in range(held.shape[0])
    ]
    for copy in get:
        copy.start()
    for index, copy in enumerate(put):
        get[index].wait()
        copy.start()
    for copy in put:
        copy.wait()


def portions_to_send(latent, portions, seq_count, cfg_count):
    frames_dev, pixels, width = latent.shape
    run_len = pixels // (portions * 2 * cfg_count * seq_count)
    if frames_dev > 1 or run_len % 8:
        mine = latent.reshape(frames_dev, portions, 2, cfg_count, seq_count, run_len, width)
        mine = lax.dynamic_index_in_dim(mine, lax.axis_index("cfg"), 3, keepdims=False)
        mine = mine.transpose(0, 1, 3, 2, 4, 5).reshape(
            frames_dev, portions, seq_count, 2 * run_len, width
        )
        return [mine[:, index] for index in range(portions)]
    view = latent.reshape(portions * 2, cfg_count, seq_count, run_len, width)
    dims = (seq_count, 2 * run_len, width)
    hbm = pl.BlockSpec(memory_space=pltpu.HBM)
    outs = pl.pallas_call(
        portion_kernel,
        in_specs=[hbm],
        out_specs=[hbm] * portions,
        out_shape=[jax.ShapeDtypeStruct(dims, latent.dtype)] * portions,
        scratch_shapes=[
            pltpu.VMEM((portions * 2, seq_count, run_len, width), latent.dtype),
            pltpu.SemaphoreType.DMA((portions * 2,)),
            pltpu.SemaphoreType.DMA((portions * 2,)),
        ],
        name="portions",
    )(view)
    return [out[None] for out in outs]


def block_kernel(
    num_ref, den_ref, x_ref, mod_ref, w_hbm, wo_hbm, wh_ref, *rest, mod_cols, part
):
    if part:
        prev_ref, *rest = rest
    out_ref, mods, normed, mixed, qkv_s, w_s, wo_s, w_sem, sem = rest
    cols = w_s.shape[2] // 3
    q_s, k_s, v_s = (qkv_s.at[:, index * cols : (index + 1) * cols] for index in range(3))
    step = pl.program_id(0)
    steps = pl.num_programs(0)
    frames, items, width = x_ref.shape
    tokens = frames * items
    per_group = GROUP // frames
    groups = tokens // GROUP

    def weight_copy(index, block):
        return pltpu.make_async_copy(
            w_hbm.at[:, pl.ds(pl.multiple_of(index * width + block * cols, cols), cols)],
            w_s.at[block, :, index * cols : (index + 1) * cols],
            w_sem.at[index, block],
        )

    def latent_group(g):
        rows = x_ref[:, g * per_group : (g + 1) * per_group, :].astype(jnp.float32)
        return rows.reshape(GROUP, width)

    def normalize(values):
        center = values - jnp.mean(values, axis=-1, keepdims=True)
        spread = jnp.mean(center * center, axis=-1, keepdims=True)
        return center * lax.rsqrt(spread + NORM_FLOOR)

    def mod_part(c, index):
        return mods[c : c + 1, index * width : (index + 1) * width]

    @pl.when(step == 0)
    def _():
        for block in range(w_s.shape[0]):
            for index in range(3):
                weight_copy(index, block).start()
        pltpu.make_async_copy(wo_hbm, wo_s, sem).start()
        pieces = mod_ref.shape[0] // 2
        for c in range(2):
            for piece in range(pieces):
                for row in range(mod_ref.shape[1]):
                    size = min(128, mod_cols - row * 128)
                    start = piece * mod_cols + row * 128
                    mods[c : c + 1, start : start + size] = mod_ref[
                        c * pieces + piece, row : row + 1, :size
                    ]
        for g in range(groups):
            base = normalize(latent_group(g))
            for c in range(2):
                value = base * (1.0 + mod_part(c, 1)) + mod_part(c, 0)
                normed[c * tokens + g * GROUP : c * tokens + (g + 1) * GROUP, :] = value.astype(
                    jnp.bfloat16
                )

    @pl.when(step == 0)
    def _():
        for index in range(3):
            weight_copy(index, step).wait()
            lanes = slice(index * cols, (index + 1) * cols)
            qkv_s[:, lanes] = jnp.dot(
                normed[...], w_s[step, :, lanes], preferred_element_type=jnp.float32
            ).astype(jnp.bfloat16)

    @pl.when(step > 0)
    def _():
        for index in range(3):
            weight_copy(index, step).wait()
        qkv_s[...] = jnp.dot(normed[...], w_s[step], preferred_element_type=jnp.float32).astype(
            jnp.bfloat16
        )

    def attend():
        row_pix = lax.broadcasted_iota(jnp.int32, (GROUP, GROUP), 0) % per_group
        col_pix = lax.broadcasted_iota(jnp.int32, (GROUP, GROUP), 1) % per_group
        same = row_pix == col_pix
        low = lax.broadcasted_iota(jnp.int32, (GROUP, 128), 1) < 64
        zero = jnp.zeros((GROUP, 128), jnp.bfloat16)
        one = jnp.ones((GROUP, 128), jnp.bfloat16)
        ones_blk = jnp.concatenate([jnp.where(low, one, zero), jnp.where(low, zero, one)], axis=0)
        rate = math.log2(math.e) / math.sqrt(64.0)

        def split_heads(value):
            return jnp.concatenate(
                [jnp.where(low, value, zero), jnp.where(low, zero, value)], axis=0
            )

        def unit(rows, lanes):
            keys = split_heads(k_s[rows, lanes])
            vals = jnp.concatenate([split_heads(v_s[rows, lanes]), ones_blk], axis=1)
            scores = lax.dot_general(
                q_s[rows, lanes], keys, (((1,), (1,)), ((), ())), preferred_element_type=jnp.float32
            )
            probs = []
            for h in range(2):
                part = jnp.where(same, scores[:, h * GROUP : (h + 1) * GROUP], -jnp.inf)
                top = jnp.max(part, axis=-1, keepdims=True)
                probs.append(jnp.exp2((part - top) * rate).astype(jnp.bfloat16))
            both = jnp.dot(
                jnp.concatenate(probs, axis=1), vals, preferred_element_type=jnp.float32
            )
            mixed[step, rows, lanes] = (both[:, :128] / both[:, 128:]).astype(jnp.bfloat16)

        for g in range(2 * groups):
            for pair in range(cols // 128):
                unit(slice(g * GROUP, (g + 1) * GROUP), slice(pair * 128, (pair + 1) * 128))

    pl.when(step >= 0)(attend)

    @pl.when(step == steps - 1)
    def _():
        pltpu.make_async_copy(wo_hbm, wo_s, sem).wait()
        guide = num_ref[...].astype(jnp.float32) / den_ref[...].astype(jnp.float32)
        preds = []
        lhs = jnp.concatenate([mixed[j] for j in range(mixed.shape[0])], axis=1)
        branch = jnp.dot(lhs, wo_s[...], preferred_element_type=jnp.float32)
        for c in range(2):
            base = jnp.concatenate([latent_group(g) for g in range(groups)], axis=0)
            residual = base + mod_part(c, 2) * branch[c * tokens : (c + 1) * tokens]
            final = normalize(residual) * (1.0 + mod_part(c, 4)) + mod_part(c, 3)
            preds.append(
                lax.dot_general(
                    final.astype(jnp.bfloat16), wh_ref[...], (((1,), (1,)), ((), ())),
                    preferred_element_type=jnp.float32,
                )
            )
        guided = preds[1] + guide * (preds[0] - preds[1])
        wide = jnp.concatenate([guided[: tokens // 2], guided[tokens // 2 :]], axis=1)
        held = items // 2
        for g in range(groups // 2):
            block = wide[g * GROUP : (g + 1) * GROUP].reshape(frames, per_group, wide.shape[1])
            block = block.astype(out_ref.dtype)
            first = part * held + g * per_group
            for copy in range(out_ref.shape[0]):
                out_ref[copy, :, first : first + per_group, :] = block
        if part:
            out_ref[:, :, : part * held, :] = prev_ref[...]


def run_block(
    guide_num, guide_den, x, mods, mod_cols, qkv_weight, out_weight, head_rows, copies, prev
):
    frames, items, width = x.shape
    tokens = frames * items
    cols = 512 if width % 512 == 0 else 256
    steps = width // cols
    out_ch = head_rows.shape[0]
    part = 0 if prev is None else prev.shape[2] // (items // 2)
    out_dims = (copies, frames, (part + 1) * (items // 2), 2 * out_ch)
    whole = lambda shape: pl.BlockSpec(shape, lambda j: (0,) * len(shape))
    flops = 2 * 2 * tokens * width * (4 * width + out_ch)
    more = [] if prev is None else [prev]
    return pl.pallas_call(
        functools.partial(block_kernel, mod_cols=mod_cols, part=part),
        grid=(steps,),
        in_specs=[
            whole((1, 1)),
            whole((1, 1)),
            whole(x.shape),
            whole(mods.shape),
            pl.BlockSpec(memory_space=pltpu.HBM),
            pl.BlockSpec(memory_space=pltpu.HBM),
            whole(head_rows.shape),
            *(whole(extra.shape) for extra in more),
        ],
        out_specs=whole(out_dims),
        out_shape=jax.ShapeDtypeStruct(out_dims, jnp.bfloat16),
        scratch_shapes=[
            pltpu.VMEM((2, 5 * width), jnp.float32),
            pltpu.VMEM((2 * tokens, width), jnp.bfloat16),
            pltpu.VMEM((steps, 2 * tokens, cols), jnp.bfloat16),
            pltpu.VMEM((2 * tokens, 3 * cols), jnp.bfloat16),
            pltpu.VMEM((steps, width, 3 * cols), jnp.bfloat16),
            pltpu.VMEM(out_weight.shape, jnp.bfloat16),
            pltpu.SemaphoreType.DMA((3, steps)),
            pltpu.SemaphoreType.DMA,
        ],
        compiler_params=pltpu.CompilerParams(vmem_limit_bytes=66_500_000),
        cost_estimate=pl.CostEstimate(
            flops=flops, bytes_accessed=8 * width * width + tokens * width * 2, transcendentals=0
        ),
        name="guided_block",
    )(
        guide_num.reshape(1, 1), guide_den.reshape(1, 1), x, mods, qkv_weight, out_weight, head_rows,
        *more
    )


def order_kernel(x_ref, out_ref, *, portions):
    devices, _, rows, lanes = x_ref.shape
    run_len = rows // portions
    out_ch = lanes // 2
    span = devices * run_len
    for p in range(portions):
        block = x_ref[:, 0, p * run_len : (p + 1) * run_len, :].astype(jnp.float32)
        turned = block.reshape(span, lanes).T
        for h in range(2):
            out_ref[0, :, (2 * p + h) * span : (2 * p + h + 1) * span] = turned[
                h * out_ch : (h + 1) * out_ch
            ]


def in_order(back, portions):
    devices, frames_dev, rows, lanes = back.shape
    run_len = rows // portions
    pixels = devices * rows * 2
    out_ch = lanes // 2
    if frames_dev > 1 or run_len % 8:
        parts = back.reshape(devices, frames_dev, portions, run_len, 2, out_ch)
        parts = parts.transpose(1, 2, 4, 0, 3, 5).reshape(frames_dev, pixels, out_ch)
        return parts.astype(jnp.float32)
    turned = pl.pallas_call(
        functools.partial(order_kernel, portions=portions),
        out_shape=jax.ShapeDtypeStruct((1, out_ch, pixels), jnp.float32),
        name="in_order",
    )(back)
    return turned.transpose(0, 2, 1)


def on_device(
    latent, text_ids, timestep, guide_num, guide_den, text_table, time_in, time_out, mod_weight,
    qkv_weight, out_weight, head_weight,
):
    frames_dev, pixels, width = latent.shape
    seq_count = lax.axis_size("seq")
    cfg_count = lax.axis_size("cfg")
    half = pixels // cfg_count
    items = half // seq_count
    frames = frames_dev * seq_count
    portions = 2
    some = items // portions
    devices = cfg_count * seq_count
    mine = portions_to_send(latent, portions, seq_count, cfg_count)

    def exchange(portion):
        got = lax.all_to_all(portion, "seq", split_axis=1, concat_axis=0, tiled=True)
        return got.reshape(frames, some, width)

    received = exchange(mine[0])

    part = conditioning_part(text_ids, time_features(timestep), text_table, time_in, time_out)
    summed = seq_sum(part, seq_count)
    cond = jax.nn.silu(summed).astype(jnp.bfloat16)
    mod_mine = jnp.dot(cond, mod_weight, preferred_element_type=jnp.float32)
    mod_mine, received = lax.optimization_barrier((mod_mine, received))
    mod_cols = mod_mine.shape[1]
    lines = -(-mod_cols // 128)
    piece = jnp.pad(mod_mine[0], (0, lines * 128 - mod_cols)).reshape(1, lines, 128)
    mods = lax.all_to_all(
        jnp.broadcast_to(piece, (devices, lines, 128)), ("cfg", "seq"),
        split_axis=0, concat_axis=0, tiled=True,
    )
    mods, rest = lax.optimization_barrier((mods, mine[1]))
    run = lambda x, prev: run_block(
        guide_num, guide_den, x, mods, mod_cols, qkv_weight, out_weight, head_weight.T, cfg_count, prev
    )
    later = exchange(rest)
    combined = run(later, run(received, None))
    out_ch = head_weight.shape[1]
    send = combined.reshape(devices, frames_dev, items // 2, 2 * out_ch)
    back = lax.all_to_all(send, ("cfg", "seq"), split_axis=0, concat_axis=0, tiled=True)
    return in_order(back, portions)


def solution(mesh):
    in_specs = (
        P("seq", None, None), P("cfg", None), P(), P(), P(), P("seq", None), P(), P(None, "seq"),
        P(None, "seq"), P(), P(), P(),
    )
    return jax.shard_map(
        on_device, mesh=mesh, in_specs=in_specs, out_specs=P("seq", None, None), check_vma=False
    )
```
